256 devices in a mesh: row: 64 (over x, z, core), col: 4 (over y).
Axes of the slice: x: 4, y: 4, z: 8, core: 2. Of those that a mesh axis runs over, the one named last changes fastest.
Arguments:
- eigvecs: float32 [16384, 512], P('row', 'col'), may hold values from -6 to 6
- reflectors: float32 [8, 256, 128, 64], P(None, ('row', 'col')), may hold values from -2 to 2, as said below
- factors: float32 [8, 256, 64, 64], P(None, ('row', 'col')), may hold values from -3 to 3, as said below
- order: int32 [8], replicated, may hold values from 0 to 7, each once
- offsets: int32 [8], replicated, may hold values from 0 to 63
Outputs:
- rotated: float32 [16384, 512], P('row', 'col')
The draws below stay inside these ranges and needn't reach their ends.
Inputs may be any that keep to these rules, and one draw needn't show every extreme that they name: `order`: a permutation of 0 .. 7. Every block map is orthogonal: with V the block of reflectors and T the block of factors, T is upper triangular and T^-1 + T^-T = V^T V. `factors`: upper triangular, paired with reflectors as promised there.
All inputs are finite; a program needn't handle non-finite values.
Results may differ from the reference program's by a relative error of at most 0.0003.
Values sent between devices are 32-bit elements; how exact they have to be, the bound alone decides.
No kernel may reach another device: no remote copies, remote signals or barrier semaphores. Data moves between devices by JAX's collectives and lax.ppermute only.
A program may use at most 64 MiB of HBM per device.

```python
import jax
import jax.numpy as jnp
from jax import lax

NB = 64
SWEEPS = 8
NBLK = 256
ORDER = 16384
VECS = 512


def build_pair(key):
    inner_key = jax.random.fold_in(key, 11)
    spread = 0.03
    identity = jnp.eye(NB, dtype=jnp.float32)
    base = jnp.concatenate([identity, -identity], 0)
    noise = jax.random.normal(inner_key, (SWEEPS, NBLK, 2 * NB, NB), jnp.float32) * spread
    householder = base + noise
    gram = jnp.einsum('abik,abil->abkl', householder, householder, precision=lax.Precision.HIGHEST)
    inverse_factor = jnp.triu(gram, 1) + gram * identity * 0.5
    triangle = lax.linalg.triangular_solve(inverse_factor, jnp.broadcast_to(identity, inverse_factor.shape), left_side=True, lower=False)
    return (householder, triangle)


def draw_reflectors(key, part):
    return build_pair(key)[0]


def draw_factors(key, part):
    return build_pair(key)[1]


def with_ends(drawn, own_key, smallest, top_value):
    longest = drawn.shape.index(max(drawn.shape))
    spots = []
    for shift in (0, 1):
        where = [jax.random.randint(jax.random.fold_in(own_key, axis), (), 0, length) for axis, length in enumerate(drawn.shape)]
        where[longest] = (where[longest] + shift) % drawn.shape[longest]
        spots.append(tuple(where))
    return drawn.at[spots[0]].set(smallest).at[spots[1]].set(top_value)


def block_scale(stream_key, extent, cuts, least, largest):
    def one(dim, shards_of):
        heights = jax.random.uniform(jax.random.fold_in(jax.random.fold_in(stream_key, 6), dim), (shards_of,), jnp.float32, least / len(cuts), largest / len(cuts))
        return jnp.repeat(jnp.exp(heights), extent[dim] // shards_of).reshape((-1,) + (1,) * (len(extent) - dim - 1))

    loudness = one(*cuts[0])
    for cut in cuts[1:]:
        loudness = loudness * one(*cut)
    return loudness


def centred(stream_key, extent, scale, limit, split=(), kind=jnp.bfloat16):
    factor_of = block_scale(stream_key, extent, split, -0.22, 0.18) if split else 1.0
    entries = jax.random.normal(stream_key, extent, jnp.float32) * scale * factor_of
    return jnp.minimum(jnp.maximum(entries, -limit), limit).astype(kind)


def setup_inputs(seed: int = 0) -> dict:
    key_list = jax.random.split(jax.random.key(seed), 6)
    return {
        "eigvecs": centred(key_list[0], (ORDER, VECS), 1.0, 6.0, ((0, 64), (1, 4)), jnp.float32),
        "reflectors": draw_reflectors(jax.random.fold_in(key_list[5], 71), 0),
        "factors": draw_factors(jax.random.fold_in(key_list[5], 71), 0),
        "order": jax.random.permutation(key_list[3], SWEEPS).astype(jnp.int32),
        "offsets": with_ends(jax.random.randint(key_list[4], (SWEEPS,), 0, NB), jax.random.fold_in(key_list[4], 1), 0, NB - 1).astype(jnp.int32),
    }


highest = lax.Precision.HIGHEST

def reflect(segment, householder, triangle):
    inner = jnp.dot(householder.T.astype(jnp.float32), segment.astype(jnp.float32), precision=highest, preferred_element_type=jnp.float32)
    inner = jnp.dot(triangle.astype(jnp.float32), inner.astype(jnp.float32), precision=highest, preferred_element_type=jnp.float32)
    return segment - jnp.dot(householder.astype(jnp.float32), inner.astype(jnp.float32), precision=highest, preferred_element_type=jnp.float32)

def reference(eigvecs, reflectors, factors, order, offsets):
    height = eigvecs.shape[0]
    columns = eigvecs.shape[1]
    number_blocks = reflectors.shape[1]
    vectors = eigvecs
    for position in range(SWEEPS):
        stored = order[position].astype(jnp.int32)
        offset = offsets[stored].astype(jnp.int32)
        house_set = lax.dynamic_index_in_dim(reflectors, stored, 0, keepdims=False)
        tri_set = lax.dynamic_index_in_dim(factors, stored, 0, keepdims=False)
        padded = jnp.concatenate([vectors, jnp.zeros((2 * NB, columns), jnp.float32)], 0)

        def advance(number, current):
            start = (offset + number * NB).astype(jnp.int32)
            segment = lax.dynamic_slice_in_dim(current, start, 2 * NB, 0)
            householder = lax.dynamic_index_in_dim(house_set, number, 0, keepdims=False)
            triangle = lax.dynamic_index_in_dim(tri_set, number, 0, keepdims=False)
            return lax.dynamic_update_slice_in_dim(current, reflect(segment, householder, triangle), start, 0)
        padded = lax.fori_loop(0, number_blocks, advance, padded)
        vectors = padded[:height]
    return vectors
```

```python
import jax
import jax.numpy as jnp
from jax import lax
from jax.sharding import Mesh
from jax.sharding import PartitionSpec as P

ROW = ("x", "z", "core")
ROW_COL = ("x", "z", "core", "col")
FUSED = 2


def dot(a, b):
    return jnp.dot(a, b, precision=lax.Precision.HIGHEST, preferred_element_type=jnp.float32)


def bdot(a, b):
    return lax.dot_general(
        a,
        b,
        (((a.ndim - 1,), (b.ndim - 2,)), ((0,), (0,))),
        precision=lax.Precision.HIGHEST,
        preferred_element_type=jnp.float32,
    )


def from_next(block):
    size = lax.axis_size(ROW)
    return lax.ppermute(block, ROW, [(i + 1, i) for i in range(size - 1)])


def from_previous(block):
    size = lax.axis_size(ROW)
    return lax.ppermute(block, ROW, [(i, i + 1) for i in range(size - 1)])


def chain(blocks, first, rest):
    width = first.shape[0]
    finished, carried = [], []
    carry = first
    for j, block in enumerate(blocks):
        out = dot(block, jnp.concatenate([carry, rest[j * width : (j + 1) * width]], 0))
        finished.append(out[:width])
        carry = out[width:]
        carried.append(carry)
    return finished, carried


def phase_maps(window, carries, blocks_a, blocks_b, off_a, off_b, last):
    width = carries[0].shape[0]
    height = 4 * width
    own = 4
    rest = lax.dynamic_slice_in_dim(window, off_a + width, 6 * width, 0)
    finished, carried = chain(blocks_a, carries[0], rest)
    out_a = carried[own - 1]
    window = lax.dynamic_update_slice_in_dim(window, jnp.concatenate(finished, 0), off_a, 0)
    window = jnp.concatenate([window[:height], jnp.where(last, 0.0, window[height:])], 0)
    rest = lax.dynamic_slice_in_dim(window, off_b + width, own * width, 0)
    if len(carries) == 2:
        first = carries[1]
    else:
        first = lax.dynamic_slice_in_dim(window, off_b, width, 0)
    finished, carried = chain(blocks_b, first, rest)
    done = jnp.concatenate(finished, 0)
    return jnp.concatenate([out_a, carried[own - 1]], 0), window, done


def local(eigvecs, reflectors, factors, order, offsets):
    height, columns = eigvecs.shape
    width = reflectors.shape[-1]
    sweeps = reflectors.shape[0]
    phases = sweeps // FUSED
    state = FUSED * width
    index = lax.axis_index(ROW)
    chip, core, plane = lax.axis_index("z"), lax.axis_index("core"), lax.axis_index("x")
    chips, planes = lax.axis_size("z"), lax.axis_size("x")
    leading = index == 0
    last = index == lax.axis_size(ROW) - 1
    span = 2 * width
    eye = jnp.eye(span, dtype=jnp.float32)

    house = jnp.take(reflectors[:, 0], order, axis=0)
    tri = jnp.take(factors[:, 0], order, axis=0)
    offs = jnp.take(offsets, order)
    block = eye - bdot(house, bdot(tri, jnp.swapaxes(house, 1, 2)))
    blocks = lax.all_gather(block, "col", axis=1)
    halo = from_next(blocks[::FUSED, :2])

    window = jnp.concatenate([eigvecs, from_next(eigvecs)], 0)

    probe = jnp.eye(state, dtype=jnp.float32)
    blank = jnp.zeros((2 * height, state), jnp.float32)
    steps, maps, responses = [], [], []
    for n in range(phases):
        a, b = FUSED * n, FUSED * n + 1
        blocks_a = [blocks[a, j] for j in range(4)] + [halo[n, j] for j in range(2)]
        blocks_b = [blocks[b, j] for j in range(4)]
        steps.append((blocks_a, blocks_b, offs[a], offs[b], last))
        out, _, done = phase_maps(blank, (probe[:width], probe[width:]), *steps[-1])
        maps.append(out)
        responses.append(done)

    mine = jnp.stack(maps)
    theirs = lax.ppermute(mine, "core", [(0, 1), (1, 0)])
    upper = core == 1
    front = jnp.where(upper, theirs, mine)
    back = jnp.where(upper, mine, theirs)
    entry = jnp.where(upper, theirs, jnp.eye(state, dtype=jnp.float32))
    joint = bdot(back, front)
    half = lax.dynamic_slice_in_dim(joint, core * width, width, 1)
    every = lax.all_gather(half, ("z", "core"), axis=1, tiled=True)

    spread, whole = [], []
    for n in range(phases):
        total = jnp.concatenate(
            [jnp.eye(state, dtype=jnp.float32), jnp.zeros((state, chips * state), jnp.float32)], 1
        )
        at_chip = total
        for k in range(chips):
            at_chip = jnp.where(k == chip, total, at_chip)
            if k:
                total = dot(every[n, k * state : (k + 1) * state], total)
            else:
                total = jnp.concatenate([every[n, :state], total[:, state:]], 1)
            total = lax.dynamic_update_slice_in_dim(
                total, jnp.eye(state, dtype=jnp.float32), (k + 1) * state, 1
            )
        spread.append(dot(entry[n], at_chip))
        whole.append(total)
    across = lax.all_to_all(
        jnp.broadcast_to(
            jnp.stack([w[:, :state] for w in whole]), (planes, phases, state, state)
        ),
        "x",
        0,
        0,
    )
    towards, entering, leaving = [], [], []
    for n in range(phases):
        total = jnp.zeros((state, planes * state), jnp.float32)
        at_plane = total
        for k in range(planes):
            at_plane = jnp.where(k == plane, total, at_plane)
            if k < planes - 1:
                if k:
                    total = dot(across[k, n], total)
                total = lax.dynamic_update_slice_in_dim(
                    total, jnp.eye(state, dtype=jnp.float32), k * state, 1
                )
        towards.append(dot(spread[n][:, :state], at_plane))
        entering.append(jnp.concatenate([spread[n][:, state:], whole[n][:, state:]], 0))

    rows = lax.broadcasted_iota(jnp.int32, (height, 1), 0)
    for n in range(phases):
        off_a, off_b = steps[n][2], steps[n][3]
        first = jnp.where(leading, lax.dynamic_slice_in_dim(window, off_a, width, 0), 0.0)
        blocks_a, blocks_b = steps[n][0], steps[n][1]
        rest = lax.dynamic_slice_in_dim(window, off_a + width, 6 * width, 0)
        finished, carried = chain(blocks_a, first, rest)
        out_a = carried[3]
        window = lax.dynamic_update_slice_in_dim(window, jnp.concatenate(finished, 0), off_a, 0)
        window = jnp.concatenate([window[:height], jnp.where(last, 0.0, window[height:])], 0)
        first = jnp.where(leading, lax.dynamic_slice_in_dim(window, off_b, width, 0), 0.0)
        rest = lax.dynamic_slice_in_dim(window, off_b + width, 4 * width, 0)
        finished, carried = chain(blocks_b, first, rest)
        partial = jnp.concatenate([out_a, carried[3]], 0)
        done = jnp.concatenate(finished, 0)

        other = lax.ppermute(partial, "core", [(0, 1), (1, 0)])
        front = jnp.where(upper, other, partial)
        back = jnp.where(upper, partial, other)
        mine_half = lax.dynamic_slice_in_dim(maps_back(maps[n], theirs[n], upper), core * width, width, 0)
        chip_half = dot(mine_half, front) + lax.dynamic_slice_in_dim(back, core * width, width, 0)
        gathered = lax.all_gather(chip_half, ("z", "core"), axis=0, tiled=True)
        both = dot(entering[n], gathered)
        carry = both[:state] + jnp.where(upper, other, 0.0)
        crossing = lax.all_to_all(
            jnp.broadcast_to(both[state:], (planes, state, columns)), "x", 0, 0
        ).reshape(planes * state, columns)
        carry = carry + dot(towards[n], crossing)
        done = done + dot(responses[n], carry)
        window = lax.dynamic_update_slice_in_dim(window, done, off_b, 0)
        before = from_previous(window[height : height + width])
        top = jnp.where((rows[:width] < off_b) & ~leading, before, window[:width])
        if n == phases - 1:
            return jnp.concatenate([top, window[width:height]], 0)
        after = from_next(window[:height])
        after = jnp.where((rows < off_b) & ~last, window[height:], after)
        window = jnp.concatenate([top, window[width:height], after], 0)


def maps_back(mine, theirs, upper):
    return jnp.where(upper, mine, theirs)


def solution(mesh):
    torus = Mesh(mesh.devices.reshape(4, 8, 2, mesh.shape["col"]), ROW_COL)
    placed = (P(ROW, "col"), P(None, ROW_COL, None, None), P(None, ROW_COL, None, None), P(), P())
    return jax.shard_map(
        local, mesh=torus, in_specs=placed, out_specs=P(ROW, "col"), check_vma=False
    )
```

```python
import functools

import jax
import jax.numpy as jnp
from jax import lax
from jax.experimental import pallas as pl
from jax.experimental.pallas import tpu as pltpu
from jax.sharding import Mesh
from jax.sharding import PartitionSpec as P

ROW = ("x", "z", "core")
ROW_COL = ("x", "z", "core", "col")
W = 64
S = 2 * W
H = 4 * W
CHIPS, PLANES = 8, 4
F32 = jnp.float32


def dot(a, b):
    return jnp.dot(a, b, precision=lax.Precision.HIGHEST, preferred_element_type=F32)


def call(body, outs, *args, smem=0, scratch=(), flops=20_000_000):
    spaces = [pl.BlockSpec(memory_space=pltpu.SMEM)] * smem
    spaces += [pl.BlockSpec(memory_space=pltpu.VMEM)] * (len(args) - smem)
    single = not isinstance(outs, list)
    shapes = [jax.ShapeDtypeStruct(o, F32) for o in ([outs] if single else outs)]
    specs = [pl.BlockSpec(memory_space=pltpu.VMEM)] * len(shapes)
    return pl.pallas_call(
        body,
        out_shape=shapes[0] if single else shapes,
        in_specs=spaces,
        out_specs=specs[0] if single else specs,
        scratch_shapes=list(scratch),
        cost_estimate=pl.CostEstimate(flops=flops, bytes_accessed=1_000_000, transcendentals=0),
        compiler_params=pltpu.CompilerParams(vmem_limit_bytes=32 * 1024 * 1024),
    )(*args)


def eye(n):
    r = lax.broadcasted_iota(jnp.int32, (n, n), 0)
    c = lax.broadcasted_iota(jnp.int32, (n, n), 1)
    return jnp.where(r == c, 1.0, 0.0).astype(F32)


def row_index():
    x, z, core = lax.axis_index("x"), lax.axis_index("z"), lax.axis_index("core")
    return (x * CHIPS + z) * 2 + core


def is_last(g):
    return g == PLANES * CHIPS * 2 - 1


def block_kernel(positions, order, house, tri, out):
    for i, p in enumerate(positions):
        v = house[order[p]]
        t = tri[order[p]]
        inner = lax.dot_general(
            t, v, (((1,), (1,)), ((), ())), precision=lax.Precision.HIGHEST, preferred_element_type=F32
        )
        h = eye(S) - dot(v, inner)
        for c in range(out.shape[0]):
            out[c, i] = h


def chain(wins, blocks, count, offset, carry):
    kept = carry
    for j in range(count):
        rest = [win[pl.ds(offset + (j + 1) * W, W), :] for win in wins]
        out = dot(blocks(j), jnp.concatenate([carry, jnp.concatenate(rest, 1)], 0))
        for k, win in enumerate(wins):
            win[pl.ds(offset + j * W, W), :] = out[:W, k * S : (k + 1) * S]
        carry = out[W:]
        if j == 3:
            kept = carry
    return kept


def maps_kernel(phases, order, offsets, blocks, halo, maps, response, win):
    last = is_last(row_index())
    r = lax.broadcasted_iota(jnp.int32, (W, S), 0)
    c = lax.broadcasted_iota(jnp.int32, (W, S), 1)
    for i, n in enumerate(phases):
        off_a, off_b = offsets[order[2 * n]], offsets[order[2 * n + 1]]
        win[...] = jnp.zeros_like(win)

        def first(j, i=i):
            return blocks[j, 2 * i] if j < 4 else halo[j - 4, i]

        def second(j, i=i):
            return blocks[j, 2 * i + 1]

        maps[i, :W] = chain([win], first, 6, off_a, jnp.where(r == c, 1.0, 0.0).astype(F32))
        win[H:, :] = jnp.where(last, 0.0, win[H:, :])
        maps[i, W:] = chain([win], second, 4, off_b, jnp.where(r + W == c, 1.0, 0.0).astype(F32))
        response[i] = win[pl.ds(off_b, H), :]


def values_kernel(n, i, order, offsets, own, halo_rows, blocks, halo, partial, win):
    g = row_index()
    last, leading = is_last(g), g == 0
    off_a, off_b = offsets[order[2 * n]], offsets[order[2 * n + 1]]
    win[:H, :] = own[:H, :]
    before = offsets[order[2 * n - 1]]
    rows = lax.broadcasted_iota(jnp.int32, (H, 1), 0)
    win[H:, :] = jnp.where((rows < before) & ~last, own[H:, :], halo_rows[...])

    def first(j):
        return blocks[j, 2 * i] if j < 4 else halo[j - 4, i]

    def second(j):
        return blocks[j, 2 * i + 1]

    partial[:W] = chain([win], first, 6, off_a, jnp.where(leading, win[pl.ds(off_a, W), :], 0.0))
    win[H:, :] = jnp.where(last, 0.0, win[H:, :])
    partial[W:] = chain([win], second, 4, off_b, jnp.where(leading, win[pl.ds(off_b, W), :], 0.0))


def join_maps_kernel(mine, theirs, half):
    core = lax.axis_index("core")
    start = pl.multiple_of(core * W, W)
    for i in range(mine.shape[0]):
        front = jnp.where(core == 1, theirs[i], mine[i])
        back = jnp.where(core == 1, mine[i, pl.ds(start, W), :], theirs[i, pl.ds(start, W), :])
        value = dot(back, front)
        if len(half.shape) == 4:
            for c in range(half.shape[0]):
                half[c, i] = value
        else:
            half[i] = value


def join_values_kernel(i, mine, theirs, partial, other, half):
    core = lax.axis_index("core")
    start = pl.multiple_of(core * W, W)
    rows = pl.ds(start, W)
    front = jnp.where(core == 1, other[...], partial[...])
    back = jnp.where(core == 1, partial[rows, :], other[rows, :])
    later = jnp.where(core == 1, mine[i, rows, :], theirs[i, rows, :])
    half[...] = dot(later, front) + back


def compose_kernel(theirs, own, swapped, entering, at_chip, whole):
    z, core = lax.axis_index("z"), lax.axis_index("core")
    for i in range(theirs.shape[0]):
        entry = jnp.where(core == 1, theirs[i], eye(S))
        to_here, to_end = jnp.zeros((S, S), F32), eye(S)
        for k in reversed(range(CHIPS)):
            both = jnp.concatenate([to_here, to_end], 0)
            entering[i, :, k * S : (k + 1) * S] = both
            low = jnp.where(core == 1, swapped[k, i], own[k, i])
            high = jnp.where(core == 1, own[k, i], swapped[k, i])
            step = jnp.concatenate([low, high], 0)
            both = dot(both, step)
            to_here = jnp.where(k == z, entry, both[:S])
            to_end = both[S:]
        at_chip[i] = to_here
        for x in range(PLANES):
            whole[x, i] = to_end


def across_kernel(at_chip, whole, towards):
    x = lax.axis_index("x")
    for i in range(at_chip.shape[0]):
        value = jnp.zeros((S, S), F32)
        for k in reversed(range(PLANES)):
            towards[i, :, k * S : (k + 1) * S] = value
            if k:
                value = dot(value, whole[k, i])
            value = jnp.where(k == x, at_chip[i], value)


def enter_kernel(i, entering, gathered, other, carry, out):
    core = lax.axis_index("core")
    both = dot(entering[i], gathered[...])
    carry[...] = both[:S] + jnp.where(core == 1, other[...], 0.0)
    for x in range(PLANES):
        out[x] = both[S:]


def finish_kernel(n, i, order, offsets, carry, towards, crossing, response, window, out):
    off_b = offsets[order[2 * n + 1]]
    total = carry[...] + dot(towards[i], crossing[...])
    out[...] = window[...]
    rows = pl.ds(off_b, H)
    out[rows, :] = out[rows, :] + dot(response[i], total)


def last_kernel(n, order, offsets, window, before, out):
    g = row_index()
    off_b = offsets[order[2 * n + 1]]
    rows = lax.broadcasted_iota(jnp.int32, (W, 1), 0)
    out[...] = window[:H, :]
    out[:W, :] = jnp.where((rows < off_b) & (g != 0), before[...], window[:W, :])


def open_kernel(order, offsets, own, halo_rows, blocks, halo, partial, window, response, win):
    g = row_index()
    last, leading = is_last(g), g == 0
    off_a, off_b = offsets[order[0]], offsets[order[1]]
    win[...] = jnp.zeros_like(win)
    window[:H, :] = own[...]
    window[H:, :] = halo_rows[...]
    r = lax.broadcasted_iota(jnp.int32, (W, S), 0)
    c = lax.broadcasted_iota(jnp.int32, (W, S), 1)
    ones = jnp.where(r == c, 1.0, 0.0).astype(F32)
    carry = jnp.concatenate([jnp.where(leading, window[pl.ds(off_a, W), :], 0.0), ones], 1)
    wins = [window, win]
    partial[:W] = chain(wins, lambda j: blocks[j, 0] if j < 4 else halo[j - 4, 0], 6, off_a, carry)
    for part in wins:
        part[H:, :] = jnp.where(last, 0.0, part[H:, :])
    ones = jnp.where(r + W == c, 1.0, 0.0).astype(F32)
    carry = jnp.concatenate([jnp.where(leading, window[pl.ds(off_b, W), :], 0.0), ones], 1)
    partial[W:] = chain(wins, lambda j: blocks[j, 1], 4, off_b, carry)
    response[...] = win[pl.ds(off_b, H), :]


def open_join_kernel(partial, other, half):
    core = lax.axis_index("core")
    rows = pl.ds(pl.multiple_of(core * W, W), W)
    front = jnp.where(core == 1, other[...], partial[...])
    back = jnp.where(core == 1, partial[rows, :], other[rows, :])
    own = jnp.concatenate([back[:, :S], jnp.zeros((W, S), F32)], 1)
    value = dot(back[:, S:], front) + own
    for c in range(half.shape[0]):
        half[c] = value


def open_enter_kernel(other, own, swapped, carry, at_chip, out):
    z, core = lax.axis_index("z"), lax.axis_index("core")
    entry = jnp.where(core == 1, other[:, S:], eye(S))
    add = jnp.where(core == 1, other[:, :S], 0.0)
    to_here, to_end = jnp.zeros((S, S), F32), eye(S)
    total = jnp.zeros((2 * S, S), F32)
    for k in reversed(range(CHIPS)):
        low = jnp.where(core == 1, swapped[k], own[k])
        high = jnp.where(core == 1, own[k], swapped[k])
        both = dot(jnp.concatenate([to_here, to_end], 0), jnp.concatenate([low, high], 0))
        total = total + both[:, :S]
        to_here = jnp.where(k == z, entry, both[:S, S:])
        to_end = both[S:, S:]
    carry[...] = total[:S] + add
    at_chip[...] = to_here
    value = jnp.concatenate([total[S:], to_end], 1)
    for x in range(PLANES):
        out[x] = value


def open_finish_kernel(order, offsets, carry, at_chip, crossing, response, window, out):
    x = lax.axis_index("x")
    off_b = offsets[order[1]]
    total = carry[...]
    value = jnp.zeros((S, S), F32)
    for k in reversed(range(PLANES)):
        step = dot(value, crossing[k])
        total = total + step[:, :S]
        value = jnp.where(k == x, at_chip[...], step[:, S:])
    out[...] = window[...]
    rows = pl.ds(off_b, H)
    out[rows, :] = out[rows, :] + dot(response[...], total)


def from_next(block):
    size = lax.axis_size(ROW)
    return lax.ppermute(block, ROW, [(i + 1, i) for i in range(size - 1)])


def from_previous(block):
    size = lax.axis_size(ROW)
    return lax.ppermute(block, ROW, [(i, i + 1) for i in range(size - 1)])


def swap(block):
    return lax.ppermute(block, "core", [(0, 1), (1, 0)])


def local(eigvecs, reflectors, factors, order, offsets):
    columns = eigvecs.shape[1]
    house, tri = reflectors[:, 0], factors[:, 0]
    phases = order.shape[0] // 2
    cols = lax.axis_size("col")

    def gather_blocks(ns, house=house, tri=tri):
        positions = [2 * n + k for n in ns for k in (0, 1)]
        copies = call(
            functools.partial(block_kernel, positions),
            (cols, len(positions), S, S),
            order, house, tri, smem=1,
        )
        return lax.all_to_all(copies, "col", 0, 0)

    def maps_of(ns, blocks):
        halo = from_next(blocks[:2, ::2])
        maps, response = call(
            functools.partial(maps_kernel, ns),
            [(len(ns), S, S), (len(ns), H, S)],
            order, offsets, blocks, halo, smem=2,
            scratch=[pltpu.VMEM((2 * H, S), F32)],
        )
        return halo, maps, response

    def compose(maps):
        count = maps.shape[0]
        theirs = swap(maps)
        copies = call(join_maps_kernel, (CHIPS, count, W, S), maps, theirs)
        own = lax.all_to_all(copies, "z", 0, 0)
        entering, at_chip, whole = call(
            compose_kernel,
            [(count, 2 * S, CHIPS * S), (count, S, S), (PLANES, count, S, S)],
            theirs, own, swap(own),
        )
        whole = lax.all_to_all(whole, "x", 0, 0)
        towards = call(across_kernel, (count, S, PLANES * S), at_chip, whole)
        return theirs, entering, towards

    halo_rows = from_next(eigvecs)
    blocks = gather_blocks([0])
    rest = list(range(1, phases))
    (later_house, later_tri), blocks = lax.optimization_barrier(((house, tri), blocks))
    later_blocks = gather_blocks(rest, later_house, later_tri)
    halo = from_next(blocks[:2, ::2])
    partial, window, response = call(
        open_kernel,
        [(S, 2 * S), (2 * H, columns), (H, S)],
        order, offsets, eigvecs, halo_rows, blocks, halo, smem=2,
        scratch=[pltpu.VMEM((2 * H, S), F32)],
    )
    other = swap(partial)
    own = lax.all_to_all(call(open_join_kernel, (CHIPS, W, 2 * S), partial, other), "z", 0, 0)
    later = maps_of(rest, later_blocks)
    carry, at_chip, out = call(
        open_enter_kernel, [(S, columns), (S, S), (PLANES, S, 2 * S)], other, own, swap(own)
    )
    crossing = lax.all_to_all(out, "x", 0, 0)
    window = call(
        open_finish_kernel, (2 * H, columns),
        order, offsets, carry, at_chip, crossing, response, window, smem=2,
    )
    halo, maps, response = later
    blocks = later_blocks
    theirs, entering, towards = compose(maps)

    for n in rest:
        i = n - 1
        halo_rows = from_next(window[:H])
        partial, window = call(
            functools.partial(values_kernel, n, i),
            [(S, columns), (2 * H, columns)],
            order, offsets, window, halo_rows, blocks, halo, smem=2,
        )
        other = swap(partial)
        half = call(
            functools.partial(join_values_kernel, i), (W, columns), maps, theirs, partial, other
        )
        gathered = lax.all_gather(half, ("z", "core"), axis=0, tiled=True)
        carry, out = call(
            functools.partial(enter_kernel, i),
            [(S, columns), (PLANES, S, columns)],
            entering, gathered, other,
        )
        crossing = lax.all_to_all(out, "x", 0, 0).reshape(PLANES * S, columns)
        window = call(
            functools.partial(finish_kernel, n, i), (2 * H, columns),
            order, offsets, carry, towards, crossing, response, window, smem=2,
        )
    before = from_previous(window[H : H + W])
    return call(
        functools.partial(last_kernel, phases - 1), (H, columns),
        order, offsets, window, before, smem=2,
    )


def solution(mesh):
    torus = Mesh(mesh.devices.reshape(PLANES, CHIPS, 2, mesh.shape["col"]), ROW_COL)
    placed = (P(ROW, "col"), P(None, ROW_COL, None, None), P(None, ROW_COL, None, None), P(), P())
    return jax.shard_map(
        local, mesh=torus, in_specs=placed, out_specs=P(ROW, "col"), check_vma=False
    )
```

```python
import functools

import jax
import jax.numpy as jnp
from jax import lax
from jax.experimental import pallas as pl
from jax.experimental.pallas import tpu as pltpu
from jax.sharding import Mesh
from jax.sharding import PartitionSpec as P

ROW = ("x", "z", "core")
ROW_COL = ("x", "z", "core", "col")
W = 64
S = 2 * W
H = 4 * W
CHIPS, PLANES = 8, 4
SHARE = (S + S - W // 2) // 2
F32 = jnp.float32


def exact(a, b, dims=(((1,), (0,)), ((), ()))):
    return lax.dot_general(a, b, dims, precision=lax.Precision.HIGHEST, preferred_element_type=F32)


def halves(a):
    high = a.astype(jnp.bfloat16)
    return high, (a - high.astype(F32)).astype(jnp.bfloat16)


def dot(a, b):
    a_high, a_low = halves(a)
    b_high, b_low = halves(b)
    return jnp.dot(
        jnp.concatenate([a_high, a_high, a_low], 1),
        jnp.concatenate([b_high, b_low, b_high], 0),
        preferred_element_type=F32,
    )


def call(body, outs, *args, smem=0, scratch=(), flops=20_000_000):
    spaces = [pl.BlockSpec(memory_space=pltpu.SMEM)] * smem
    spaces += [pl.BlockSpec(memory_space=pltpu.VMEM)] * (len(args) - smem)
    single = not isinstance(outs, list)
    shapes = [jax.ShapeDtypeStruct(o, F32) for o in ([outs] if single else outs)]
    specs = [pl.BlockSpec(memory_space=pltpu.VMEM)] * len(shapes)
    return pl.pallas_call(
        body,
        out_shape=shapes[0] if single else shapes,
        in_specs=spaces,
        out_specs=specs[0] if single else specs,
        scratch_shapes=list(scratch),
        cost_estimate=pl.CostEstimate(flops=flops, bytes_accessed=1_000_000, transcendentals=0),
        compiler_params=pltpu.CompilerParams(vmem_limit_bytes=32 * 1024 * 1024),
    )(*args)


def eye(n):
    r = lax.broadcasted_iota(jnp.int32, (n, n), 0)
    c = lax.broadcasted_iota(jnp.int32, (n, n), 1)
    return jnp.where(r == c, 1.0, 0.0).astype(F32)


def row_index():
    x, z, core = lax.axis_index("x"), lax.axis_index("z"), lax.axis_index("core")
    return (x * CHIPS + z) * 2 + core


def is_last(g):
    return g == PLANES * CHIPS * 2 - 1


def block_kernel(positions, order, house, tri, out):
    for i, p in enumerate(positions):
        v = house[order[p], 0]
        t = tri[order[p], 0]
        h = eye(S) - exact(v, exact(t, v, (((1,), (1,)), ((), ()))))
        if len(out.shape) == 4:
            for c in range(out.shape[0]):
                out[c, i] = h
        else:
            out[i] = h


def pick_kernel(part0, part1, part2, part3, blocks, head):
    parts = (part0, part1, part2, part3)
    for j in range(4):
        back = lax.rem(lax.axis_index("col") + 4 - j, 4)
        for i in range(part0.shape[0]):
            block = part0[i]
            for k in (1, 2, 3):
                block = jnp.where(back == k, parts[k][i], block)
            blocks[j, i] = block
            if j < 2 and i % 2 == 0:
                head[j, i // 2] = block


def chain(wins, blocks, count, offset, carry):
    kept = carry
    for j in range(count):
        rest = [win[pl.ds(offset + (j + 1) * W, W), :] for win in wins]
        out = dot(blocks(j), jnp.concatenate([carry, jnp.concatenate(rest, 1)], 0))
        for k, win in enumerate(wins):
            win[pl.ds(offset + j * W, W), :] = out[:W, k * S : (k + 1) * S]
        carry = out[W:]
        if j == 3:
            kept = carry
    return kept


def phase_kernel(n, i, order, offsets, own, halo_rows, blocks, halo, partial, window, response, win):
    g = row_index()
    last, leading = is_last(g), g == 0
    off_a, off_b = offsets[order[2 * n]], offsets[order[2 * n + 1]]
    win[...] = jnp.zeros_like(win)
    window[:H, :] = own[:H, :]
    if n:
        before = offsets[order[2 * n - 1]]
        rows = lax.broadcasted_iota(jnp.int32, (H, 1), 0)
        window[H:, :] = jnp.where((rows < before) & ~last, own[H:, :], halo_rows[...])
    else:
        window[H:, :] = halo_rows[...]
    r = lax.broadcasted_iota(jnp.int32, (W, S), 0)
    c = lax.broadcasted_iota(jnp.int32, (W, S), 1)
    wins = [window, win]

    def first(j):
        return blocks[j, 2 * i] if j < 4 else halo[j - 4, i]

    def second(j):
        return blocks[j, 2 * i + 1]

    ones = jnp.where(r == c, 1.0, 0.0).astype(F32)
    carry = jnp.concatenate([jnp.where(leading, window[pl.ds(off_a, W), :], 0.0), ones], 1)
    partial[:W] = chain(wins, first, 6, off_a, carry)
    for part in wins:
        part[H:, :] = jnp.where(last, 0.0, part[H:, :])
    ones = jnp.where(r + W == c, 1.0, 0.0).astype(F32)
    carry = jnp.concatenate([jnp.where(leading, window[pl.ds(off_b, W), :], 0.0), ones], 1)
    partial[W:] = chain(wins, second, 4, off_b, carry)
    response[...] = win[pl.ds(off_b, H), :]


def packed(step):
    return jnp.concatenate([step[:W // 2, :W], step[W // 2 : W, :W]], 1)


def unpacked(top, bottom):
    square = jnp.concatenate([top[:, :W], top[:, W:]], 0)
    return jnp.concatenate([jnp.concatenate([square, jnp.zeros_like(square)], 1), bottom], 0)


CUT = SHARE - W // 2


def join_kernel(partial, other, share):
    upper = lax.axis_index("core") == 1
    front = jnp.where(upper, other[...], partial[...])
    back = jnp.where(upper, partial[...], other[...])
    value = dot(back[:, S:], front)
    rows, step = value[:, :S] + back[:, :S], value[:, S:]
    low = jnp.concatenate([packed(step), rows[:CUT]], 0)
    high = jnp.concatenate([step[W:], rows[CUT:]], 0)
    share[...] = jnp.where(upper, high, low)


def enter_kernel(other, shares, carry, at_chip, out):
    z, upper = lax.axis_index("z"), lax.axis_index("core") == 1
    entry = jnp.where(upper, other[:, S:], eye(S))
    add = jnp.where(upper, other[:, :S], 0.0)
    to_here, to_end = jnp.zeros((S, S), F32), eye(S)
    total = jnp.zeros((2 * S, S), F32)
    for k in reversed(range(CHIPS)):
        low = shares[2 * k * SHARE : (2 * k + 1) * SHARE]
        high = shares[(2 * k + 1) * SHARE : (2 * k + 2) * SHARE]
        step = unpacked(low[: W // 2], high[:W])
        rows = jnp.concatenate([low[W // 2 :], high[W:]], 0)
        both = dot(jnp.concatenate([to_here, to_end], 0), jnp.concatenate([rows, step], 1))
        total = total + both[:, :S]
        to_here = jnp.where(k == z, entry, both[:S, S:])
        to_end = both[S:, S:]
    carry[...] = total[:S] + add
    at_chip[...] = to_here
    value = jnp.concatenate([total[S:], packed(to_end), to_end[W:]], 0)
    for x in range(PLANES):
        out[x] = value


def finish_kernel(n, order, offsets, carry, at_chip, crossing, response, window, out):
    x = lax.axis_index("x")
    off_b = offsets[order[2 * n + 1]]
    total = carry[...]
    value = jnp.zeros((S, S), F32)
    for k in reversed(range(PLANES)):
        step = unpacked(crossing[k, S : S + W // 2], crossing[k, S + W // 2 :])
        both = dot(value, jnp.concatenate([crossing[k, :S], step], 1))
        total = total + both[:, :S]
        value = jnp.where(k == x, at_chip[...], both[:, S:])
    out[...] = window[...]
    rows = pl.ds(off_b, H)
    out[rows, :] = out[rows, :] + dot(response[...], total)


def last_kernel(n, order, offsets, window, before, out):
    g = row_index()
    off_b = offsets[order[2 * n + 1]]
    rows = lax.broadcasted_iota(jnp.int32, (W, 1), 0)
    out[...] = window[:H, :]
    out[:W, :] = jnp.where((rows < off_b) & (g != 0), before[...], window[:W, :])


def from_next(block):
    size = lax.axis_size(ROW)
    return lax.ppermute(block, ROW, [(i + 1, i) for i in range(size - 1)])


def from_previous(block):
    size = lax.axis_size(ROW)
    return lax.ppermute(block, ROW, [(i, i + 1) for i in range(size - 1)])


def swap(block):
    return lax.ppermute(block, "core", [(0, 1), (1, 0)])


def local(eigvecs, reflectors, factors, order, offsets):
    columns = eigvecs.shape[1]
    phases = order.shape[0] // 2
    cols = lax.axis_size("col")

    halo_rows = from_next(eigvecs)
    block = call(
        functools.partial(block_kernel, [0, 1]), (cols, 2, S, S), order, reflectors, factors, smem=1
    )
    blocks = lax.all_to_all(block, "col", 0, 0)
    later = call(
        functools.partial(block_kernel, list(range(2, 2 * phases))),
        (2 * phases - 2, S, S),
        order, reflectors, factors, smem=1,
    )
    halo = from_next(blocks[:2, ::2])
    later, halo, halo_rows = lax.optimization_barrier((later, halo, halo_rows))
    parts = [later] + [
        lax.ppermute(later, "col", [(c, (c + d) % cols) for c in range(cols)]) for d in (1, 2, 3)
    ]
    window = eigvecs
    for n in range(phases):
        partial, window, response = call(
            functools.partial(phase_kernel, n, max(n - 1, 0)),
            [(S, 2 * S), (2 * H, columns), (H, S)],
            order, offsets, window, halo_rows, blocks, halo, smem=2,
            scratch=[pltpu.VMEM((2 * H, S), F32)],
        )
        other = swap(partial)
        share = call(join_kernel, (SHARE, columns), partial, other)
        shares = lax.all_gather(share, ("z", "core"), axis=0, tiled=True)
        carry, at_chip, out = call(
            enter_kernel,
            [(S, columns), (S, S), (PLANES, 2 * SHARE, S)],
            other, shares,
        )
        crossing = lax.all_to_all(out, "x", 0, 0)
        if n == 0:
            crossing, parts = lax.optimization_barrier((crossing, parts))
            blocks, head = call(
                pick_kernel,
                [(cols, 2 * phases - 2, S, S), (2, phases - 1, S, S)],
                *parts,
            )
            halo = from_next(head)
        window = call(
            functools.partial(finish_kernel, n), (2 * H, columns),
            order, offsets, carry, at_chip, crossing, response, window, smem=2,
        )
        if n < phases - 1:
            halo_rows = from_next(window[:H])
    before = from_previous(window[H : H + W])
    return call(
        functools.partial(last_kernel, phases - 1), (H, columns),
        order, offsets, window, before, smem=2,
    )


def solution(mesh):
    torus = Mesh(mesh.devices.reshape(PLANES, CHIPS, 2, mesh.shape["col"]), ROW_COL)
    placed = (P(ROW, "col"), P(None, ROW_COL, None, None), P(None, ROW_COL, None, None), P(), P())
    return jax.shard_map(
        local, mesh=torus, in_specs=placed, out_specs=P(ROW, "col"), check_vma=False
    )
```

```python
import functools

import jax
import jax.numpy as jnp
from jax import lax
from jax.experimental import pallas as pl
from jax.experimental.pallas import tpu as pltpu
from jax.sharding import Mesh
from jax.sharding import PartitionSpec as P

ROW = ("x", "z", "core")
ROW_COL = ("x", "z", "core", "col")
W = 64
S = 2 * W
H = 4 * W
CHIPS, PLANES = 8, 4
SHARE = (S + S - W // 2) // 2
F32 = jnp.float32


def exact(a, b, axis):
    return lax.dot_general(
        a,
        b,
        (((axis,), (0,)), ((), ())),
        precision=lax.Precision.HIGHEST,
        preferred_element_type=F32,
    )


def halves(a):
    high = a.astype(jnp.bfloat16)
    return high, (a - high.astype(F32)).astype(jnp.bfloat16)


def dot(a, b):
    a_high, a_low = halves(a)
    b_high, b_low = halves(b)
    return jnp.dot(
        jnp.concatenate([a_high, a_high, a_low], 1),
        jnp.concatenate([b_high, b_low, b_high], 0),
        preferred_element_type=F32,
    )


def call(body, outs, *args, smem=0, hbm=0, scratch=(), flops=20_000_000, limit=32):
    spaces = [pl.BlockSpec(memory_space=pltpu.SMEM)] * smem
    spaces += [pl.BlockSpec(memory_space=pltpu.HBM)] * hbm
    spaces += [pl.BlockSpec(memory_space=pltpu.VMEM)] * (len(args) - smem - hbm)
    single = not isinstance(outs, list)
    shapes = [jax.ShapeDtypeStruct(o, F32) for o in ([outs] if single else outs)]
    specs = [pl.BlockSpec(memory_space=pltpu.VMEM)] * len(shapes)
    return pl.pallas_call(
        body,
        out_shape=shapes[0] if single else shapes,
        in_specs=spaces,
        out_specs=specs[0] if single else specs,
        scratch_shapes=list(scratch),
        cost_estimate=pl.CostEstimate(flops=flops, bytes_accessed=1_000_000, transcendentals=0),
        compiler_params=pltpu.CompilerParams(vmem_limit_bytes=limit * 1024 * 1024),
    )(*args)


def eye(n):
    r = lax.broadcasted_iota(jnp.int32, (n, n), 0)
    c = lax.broadcasted_iota(jnp.int32, (n, n), 1)
    return jnp.where(r == c, 1.0, 0.0).astype(F32)


def row_index():
    x, z, core = lax.axis_index("x"), lax.axis_index("z"), lax.axis_index("core")
    return (x * CHIPS + z) * 2 + core


def is_last(g):
    return g == PLANES * CHIPS * 2 - 1


def block_kernel(positions, order, house, tri, out, v, t, sems):
    copies = []
    for i, p in enumerate(positions):
        copies.append(pltpu.make_async_copy(house.at[order[p], 0], v.at[i], sems.at[i, 0]))
        copies.append(pltpu.make_async_copy(tri.at[order[p], 0], t.at[i], sems.at[i, 1]))
    for copy in copies:
        copy.start()
    for copy in copies:
        copy.wait()
    for i in range(len(positions)):
        h = eye(S) - exact(v[i], exact(t[i], v[i], 1), 0)
        if len(out.shape) == 4:
            for c in range(out.shape[0]):
                out[c, i] = h
        else:
            out[i] = h


def make_blocks(positions, shape, order, house, tri):
    count = len(positions)
    return call(
        functools.partial(block_kernel, positions), shape, order, house, tri, smem=1, hbm=2,
        limit=60,
        scratch=[
            pltpu.VMEM((count, W, S), F32),
            pltpu.VMEM((count, W, W), F32),
            pltpu.SemaphoreType.DMA((count, 2)),
        ],
    )


def pick_kernel(part0, part1, part2, part3, blocks, head):
    parts = (part0, part1, part2, part3)
    for j in range(4):
        back = lax.rem(lax.axis_index("col") + 4 - j, 4)
        for i in range(part0.shape[0]):
            block = part0[i]
            for k in (1, 2, 3):
                block = jnp.where(back == k, parts[k][i], block)
            blocks[j, i] = block
            if j < 2 and i % 2 == 0:
                head[j, i // 2] = block


def chain(wins, blocks, count, offset, carry):
    kept = carry
    added = []
    for j in range(count):
        rest = [win[pl.ds(offset + (j + 1) * W, W), :] for win in wins]
        added.append(dot(blocks(j)[:, W:], jnp.concatenate(rest, 1)))
    for j in range(count):
        out = dot(blocks(j)[:, :W], carry) + added[j]
        for k, win in enumerate(wins):
            win[pl.ds(offset + j * W, W), :] = out[:W, k * S : (k + 1) * S]
        carry = out[W:]
        if j == 3:
            kept = carry
    return kept


def phase_kernel(n, i, order, offsets, own, halo_rows, blocks, halo, partial, window, response, win):
    g = row_index()
    last, leading = is_last(g), g == 0
    off_a, off_b = offsets[order[2 * n]], offsets[order[2 * n + 1]]
    win[...] = jnp.zeros_like(win)
    window[:H, :] = own[:H, :]
    if n:
        before = offsets[order[2 * n - 1]]
        rows = lax.broadcasted_iota(jnp.int32, (H, 1), 0)
        window[H:, :] = jnp.where((rows < before) & ~last, own[H:, :], halo_rows[...])
    else:
        window[H:, :] = halo_rows[...]
    r = lax.broadcasted_iota(jnp.int32, (W, S), 0)
    c = lax.broadcasted_iota(jnp.int32, (W, S), 1)
    wins = [window, win]

    def first(j):
        return blocks[j, 2 * i] if j < 4 else halo[j - 4, i]

    def second(j):
        return blocks[j, 2 * i + 1]

    ones = jnp.where(r == c, 1.0, 0.0).astype(F32)
    carry = jnp.concatenate([jnp.where(leading, window[pl.ds(off_a, W), :], 0.0), ones], 1)
    partial[:W] = chain(wins, first, 6, off_a, carry)
    for part in wins:
        part[H:, :] = jnp.where(last, 0.0, part[H:, :])
    ones = jnp.where(r + W == c, 1.0, 0.0).astype(F32)
    carry = jnp.concatenate([jnp.where(leading, window[pl.ds(off_b, W), :], 0.0), ones], 1)
    partial[W:] = chain(wins, second, 4, off_b, carry)
    response[...] = win[pl.ds(off_b, H), :]


def packed(step):
    return jnp.concatenate([step[:W // 2, :W], step[W // 2 : W, :W]], 1)


def unpacked(top, bottom):
    square = jnp.concatenate([top[:, :W], top[:, W:]], 0)
    return jnp.concatenate([jnp.concatenate([square, jnp.zeros_like(square)], 1), bottom], 0)


CUT = SHARE - W // 2


def join_kernel(partial, other, share):
    upper = lax.axis_index("core") == 1
    front = jnp.where(upper, other[...], partial[...])
    back = jnp.where(upper, partial[...], other[...])
    value = dot(back[:, S:], front)
    rows, step = value[:, :S] + back[:, :S], value[:, S:]
    low = jnp.concatenate([packed(step), rows[:CUT]], 0)
    high = jnp.concatenate([step[W:], rows[CUT:]], 0)
    share[...] = jnp.where(upper, high, low)


def enter_kernel(other, shares, carry, at_chip, out):
    z, upper = lax.axis_index("z"), lax.axis_index("core") == 1
    entry = jnp.where(upper, other[:, S:], eye(S))
    add = jnp.where(upper, other[:, :S], 0.0)
    for k in reversed(range(CHIPS)):
        low = shares[2 * k * SHARE : (2 * k + 1) * SHARE]
        high = shares[(2 * k + 1) * SHARE : (2 * k + 2) * SHARE]
        step = unpacked(low[: W // 2], high[:W])
        rows = jnp.concatenate([low[W // 2 :], high[W:]], 0)
        if k == CHIPS - 1:
            total = jnp.concatenate([jnp.zeros_like(rows), rows], 0)
            to_here, to_end = jnp.where(k == z, entry, 0.0), step
            continue
        both = dot(jnp.concatenate([to_here, to_end], 0), jnp.concatenate([rows, step], 1))
        total = total + both[:, :S]
        to_here = jnp.where(k == z, entry, both[:S, S:])
        to_end = both[S:, S:]
    carry[...] = total[:S] + add
    at_chip[...] = to_here
    value = jnp.concatenate([total[S:], packed(to_end), to_end[W:]], 0)
    for x in range(PLANES):
        out[x] = value


def finish_kernel(n, order, offsets, carry, at_chip, crossing, response, window, out):
    x = lax.axis_index("x")
    off_b = offsets[order[2 * n + 1]]
    total = carry[...]
    value = jnp.where(x == PLANES - 1, at_chip[...], 0.0)
    for k in reversed(range(PLANES - 1)):
        step = unpacked(crossing[k, S : S + W // 2], crossing[k, S + W // 2 :])
        both = dot(value, jnp.concatenate([crossing[k, :S], step], 1))
        total = total + both[:, :S]
        value = jnp.where(k == x, at_chip[...], both[:, S:])
    out[...] = window[...]
    rows = pl.ds(off_b, H)
    out[rows, :] = out[rows, :] + dot(response[...], total)


def last_kernel(n, order, offsets, window, before, out):
    g = row_index()
    off_b = offsets[order[2 * n + 1]]
    rows = lax.broadcasted_iota(jnp.int32, (W, 1), 0)
    out[...] = window[:H, :]
    out[:W, :] = jnp.where((rows < off_b) & (g != 0), before[...], window[:W, :])


def from_next(block):
    size = lax.axis_size(ROW)
    return lax.ppermute(block, ROW, [(i + 1, i) for i in range(size - 1)])


def from_previous(block):
    size = lax.axis_size(ROW)
    return lax.ppermute(block, ROW, [(i, i + 1) for i in range(size - 1)])


def swap(block):
    return lax.ppermute(block, "core", [(0, 1), (1, 0)])


def local(eigvecs, reflectors, factors, order, offsets):
    columns = eigvecs.shape[1]
    phases = order.shape[0] // 2
    cols = lax.axis_size("col")

    halo_rows = from_next(eigvecs)
    reflectors = jnp.swapaxes(reflectors, 2, 3)
    block = make_blocks([0, 1], (cols, 2, S, S), order, reflectors, factors)
    blocks = lax.all_to_all(block, "col", 0, 0)
    later = make_blocks(
        list(range(2, 2 * phases)), (2 * phases - 2, S, S), order, reflectors, factors
    )
    later, blocks = lax.optimization_barrier((later, blocks))
    halo = from_next(blocks[:2, ::2])
    parts = [later] + [
        lax.ppermute(later, "col", [(c, (c + d) % cols) for c in range(cols)]) for d in (1, 2, 3)
    ]
    window = eigvecs
    for n in range(phases):
        partial, window, response = call(
            functools.partial(phase_kernel, n, max(n - 1, 0)),
            [(S, 2 * S), (2 * H, columns), (H, S)],
            order, offsets, window, halo_rows, blocks, halo, smem=2,
            scratch=[pltpu.VMEM((2 * H, S), F32)],
        )
        other = swap(partial)
        share = call(join_kernel, (SHARE, columns), partial, other)
        shares = lax.all_gather(share, ("z", "core"), axis=0, tiled=True)
        carry, at_chip, out = call(
            enter_kernel,
            [(S, columns), (S, S), (PLANES, 2 * SHARE, S)],
            other, shares,
        )
        crossing = lax.all_to_all(out, "x", 0, 0)
        if n == 0:
            crossing, parts = lax.optimization_barrier((crossing, parts))
            blocks, head = call(
                pick_kernel,
                [(cols, 2 * phases - 2, S, S), (2, phases - 1, S, S)],
                *parts,
            )
            halo = from_next(head)
        window = call(
            functools.partial(finish_kernel, n), (2 * H, columns),
            order, offsets, carry, at_chip, crossing, response, window, smem=2,
        )
        if n < phases - 1:
            halo_rows = from_next(window[:H])
    before = from_previous(window[H : H + W])
    return call(
        functools.partial(last_kernel, phases - 1), (H, columns),
        order, offsets, window, before, smem=2,
    )


def solution(mesh):
    torus = Mesh(mesh.devices.reshape(PLANES, CHIPS, 2, mesh.shape["col"]), ROW_COL)
    placed = (P(ROW, "col"), P(None, ROW_COL, None, None), P(None, ROW_COL, None, None), P(), P())
    return jax.shard_map(
        local, mesh=torus, in_specs=placed, out_specs=P(ROW, "col"), check_vma=False
    )
```

```python
import functools

import jax
import jax.numpy as jnp
from jax import lax
from jax.experimental import pallas as pl
from jax.experimental.pallas import tpu as pltpu
from jax.sharding import Mesh
from jax.sharding import PartitionSpec as P

ROW = ("x", "z", "core")
ROW_COL = ("x", "z", "core", "col")
W = 64
S = 2 * W
H = 4 * W
CHIPS, PLANES = 8, 4
SHARE = (S + S - W // 2) // 2
F32 = jnp.float32


def exact(a, b, axis):
    return lax.dot_general(
        a,
        b,
        (((axis,), (0,)), ((), ())),
        precision=lax.Precision.HIGHEST,
        preferred_element_type=F32,
    )


def halves(a):
    high = a.astype(jnp.bfloat16)
    return high, (a - high.astype(F32)).astype(jnp.bfloat16)


def dot(a, b):
    a_high, a_low = halves(a)
    b_high, b_low = halves(b)
    return jnp.dot(
        jnp.concatenate([a_high, a_high, a_low], 1),
        jnp.concatenate([b_high, b_low, b_high], 0),
        preferred_element_type=F32,
    )


def call(body, outs, *args, smem=0, hbm=0, scratch=(), flops=20_000_000, limit=32):
    spaces = [pl.BlockSpec(memory_space=pltpu.SMEM)] * smem
    spaces += [pl.BlockSpec(memory_space=pltpu.HBM)] * hbm
    spaces += [pl.BlockSpec(memory_space=pltpu.VMEM)] * (len(args) - smem - hbm)
    single = not isinstance(outs, list)
    shapes = [jax.ShapeDtypeStruct(o, F32) for o in ([outs] if single else outs)]
    specs = [pl.BlockSpec(memory_space=pltpu.VMEM)] * len(shapes)
    return pl.pallas_call(
        body,
        out_shape=shapes[0] if single else shapes,
        in_specs=spaces,
        out_specs=specs[0] if single else specs,
        scratch_shapes=list(scratch),
        cost_estimate=pl.CostEstimate(flops=flops, bytes_accessed=1_000_000, transcendentals=0),
        compiler_params=pltpu.CompilerParams(vmem_limit_bytes=limit * 1024 * 1024),
    )(*args)


def eye(n):
    r = lax.broadcasted_iota(jnp.int32, (n, n), 0)
    c = lax.broadcasted_iota(jnp.int32, (n, n), 1)
    return jnp.where(r == c, 1.0, 0.0).astype(F32)


def row_index():
    x, z, core = lax.axis_index("x"), lax.axis_index("z"), lax.axis_index("core")
    return (x * CHIPS + z) * 2 + core


def is_last(g):
    return g == PLANES * CHIPS * 2 - 1


def block_kernel(positions, order, house, tri, out, v, t, sems):
    copies = []
    for i, p in enumerate(positions):
        copies.append(pltpu.make_async_copy(house.at[order[p], 0], v.at[i], sems.at[i, 0]))
        copies.append(pltpu.make_async_copy(tri.at[order[p], 0], t.at[i], sems.at[i, 1]))
    for copy in copies:
        copy.start()
    for copy in copies:
        copy.wait()
    for i in range(len(positions)):
        h = eye(S) - exact(v[i], exact(t[i], v[i], 1), 0)
        if len(out.shape) == 4:
            for c in range(out.shape[0]):
                out[c, i] = h
        else:
            out[i] = h


def make_blocks(positions, shape, order, house, tri):
    count = len(positions)
    return call(
        functools.partial(block_kernel, positions), shape, order, house, tri, smem=1, hbm=2,
        limit=60,
        scratch=[
            pltpu.VMEM((count, W, S), F32),
            pltpu.VMEM((count, W, W), F32),
            pltpu.SemaphoreType.DMA((count, 2)),
        ],
    )


def pick_kernel(part0, part1, part2, part3, blocks, head):
    parts = (part0, part1, part2, part3)
    for j in range(4):
        back = lax.rem(lax.axis_index("col") + 4 - j, 4)
        for i in range(part0.shape[0]):
            block = part0[i]
            for k in (1, 2, 3):
                block = jnp.where(back == k, parts[k][i], block)
            blocks[j, i] = block
            if j < 2 and i % 2 == 0:
                head[j, i // 2] = block


def chain(wins, blocks, count, offset, carry, fresh=0):
    kept = carry
    added = []
    used = wins[: len(wins) - fresh]
    for j in range(count):
        rest = [win[pl.ds(offset + (j + 1) * W, W), :] for win in used]
        add = dot(blocks(j)[:, W:], jnp.concatenate(rest, 1))
        if fresh:
            add = jnp.concatenate([add, jnp.zeros((S, fresh * S), F32)], 1)
        added.append(add)
    for j in range(count):
        out = dot(blocks(j)[:, :W], carry) + added[j]
        for k, win in enumerate(wins):
            win[pl.ds(offset + j * W, W), :] = out[:W, k * S : (k + 1) * S]
        carry = out[W:]
        if j == 3:
            kept = carry
    return kept


def phase_kernel(n, i, order, offsets, own, halo_rows, blocks, halo, partial, window, response, win):
    g = row_index()
    last, leading = is_last(g), g == 0
    off_a, off_b = offsets[order[2 * n]], offsets[order[2 * n + 1]]
    win[...] = jnp.zeros_like(win)
    window[:H, :] = own[:H, :]
    if n:
        before = offsets[order[2 * n - 1]]
        rows = lax.broadcasted_iota(jnp.int32, (H, 1), 0)
        window[H:, :] = jnp.where((rows < before) & ~last, own[H:, :], halo_rows[...])
    else:
        window[H:, :] = halo_rows[...]
    r = lax.broadcasted_iota(jnp.int32, (W, S), 0)
    c = lax.broadcasted_iota(jnp.int32, (W, S), 1)
    wins = [window, win]

    def first(j):
        return blocks[j, 2 * i] if j < 4 else halo[j - 4, i]

    def second(j):
        return blocks[j, 2 * i + 1]

    ones = jnp.where(r == c, 1.0, 0.0).astype(F32)
    carry = jnp.concatenate([jnp.where(leading, window[pl.ds(off_a, W), :], 0.0), ones], 1)
    partial[:W] = chain(wins, first, 6, off_a, carry, fresh=1)
    for part in wins:
        part[H:, :] = jnp.where(last, 0.0, part[H:, :])
    ones = jnp.where(r + W == c, 1.0, 0.0).astype(F32)
    carry = jnp.concatenate([jnp.where(leading, window[pl.ds(off_b, W), :], 0.0), ones], 1)
    partial[W:] = chain(wins, second, 4, off_b, carry)
    response[...] = win[pl.ds(off_b, H), :]


def packed(step):
    return jnp.concatenate([step[:W // 2, :W], step[W // 2 : W, :W]], 1)


def unpacked(top, bottom):
    square = jnp.concatenate([top[:, :W], top[:, W:]], 0)
    return jnp.concatenate([jnp.concatenate([square, jnp.zeros_like(square)], 1), bottom], 0)


CUT = SHARE - W // 2


def join_kernel(partial, other, share):
    upper = lax.axis_index("core") == 1
    front = jnp.where(upper, other[...], partial[...])
    back = jnp.where(upper, partial[...], other[...])
    value = dot(back[:, S:], front)
    rows, step = value[:, :S] + back[:, :S], value[:, S:]
    low = jnp.concatenate([packed(step), rows[:CUT]], 0)
    high = jnp.concatenate([step[W:], rows[CUT:]], 0)
    share[...] = jnp.where(upper, high, low)


def after(later, earlier):
    own = jnp.concatenate([later[:, :S], jnp.zeros((S, S), F32)], 1)
    return dot(later[:, S:], earlier) + own


def enter_kernel(other, shares, carry, at_chip, out):
    z, upper = lax.axis_index("z"), lax.axis_index("core") == 1
    same = jnp.concatenate([jnp.zeros((S, S), F32), eye(S)], 1)
    chips = []
    for k in range(CHIPS):
        low = shares[2 * k * SHARE : (2 * k + 1) * SHARE]
        high = shares[(2 * k + 1) * SHARE : (2 * k + 2) * SHARE]
        step = unpacked(low[: W // 2], high[:W])
        rows = jnp.concatenate([low[W // 2 :], high[W:]], 0)
        chips.append(jnp.concatenate([rows, step], 1))
    pairs = [after(chips[k + 1], chips[k]) for k in range(0, CHIPS, 2)]
    four, two, one = z >= 4, lax.rem(z, 4) >= 2, lax.rem(z, 2) == 1
    single = jnp.where(
        four, jnp.where(two, chips[6], chips[4]), jnp.where(two, chips[2], chips[0])
    )
    nearest = after(jnp.where(upper, other[...], same), jnp.where(one, single, same))
    pair = jnp.where(two, jnp.where(four, pairs[2], pairs[0]), same)
    front = after(pairs[1], pairs[0])
    back = after(pairs[3], pairs[2])
    here = after(after(nearest, pair), jnp.where(four, front, same))
    carry[...] = here[:, :S]
    at_chip[...] = here[:, S:]
    total = after(back, front)
    value = jnp.concatenate([total[:, :S], packed(total[:, S:]), total[W:, S:]], 0)
    for x in range(PLANES):
        out[x] = value


def finish_kernel(n, order, offsets, carry, at_chip, crossing, response, window, out):
    x = lax.axis_index("x")
    off_b = offsets[order[2 * n + 1]]

    def plane(k):
        step = unpacked(crossing[k, S : S + W // 2], crossing[k, S + W // 2 :])
        return crossing[k, :S], step

    (rows0, _), (rows1, step1), (rows2, step2) = plane(0), plane(1), plane(2)
    out[...] = window[...]
    entry = jnp.where(x == 0, 0.0, at_chip[...])
    third = dot(entry, jnp.concatenate([rows2, step2], 1))
    through = jnp.where(x == 3, third[:, S:], entry)
    arrived = jnp.where(x == 1, rows0, rows1 + dot(step1, rows0))
    total = carry[...] + dot(through, arrived) + jnp.where(x == 3, third[:, :S], 0.0)
    rows = pl.ds(off_b, H)
    out[rows, :] = out[rows, :] + dot(response[...], total)


def last_kernel(n, order, offsets, window, before, out):
    g = row_index()
    off_b = offsets[order[2 * n + 1]]
    rows = lax.broadcasted_iota(jnp.int32, (W, 1), 0)
    out[...] = window[:H, :]
    out[:W, :] = jnp.where((rows < off_b) & (g != 0), before[...], window[:W, :])


def from_next(block):
    size = lax.axis_size(ROW)
    return lax.ppermute(block, ROW, [(i + 1, i) for i in range(size - 1)])


def from_previous(block):
    size = lax.axis_size(ROW)
    return lax.ppermute(block, ROW, [(i, i + 1) for i in range(size - 1)])


def swap(block):
    return lax.ppermute(block, "core", [(0, 1), (1, 0)])


def local(eigvecs, reflectors, factors, order, offsets):
    columns = eigvecs.shape[1]
    phases = order.shape[0] // 2
    cols = lax.axis_size("col")

    halo_rows = from_next(eigvecs)
    reflectors = jnp.swapaxes(reflectors, 2, 3)
    block = make_blocks([0, 1], (cols, 2, S, S), order, reflectors, factors)
    blocks = lax.all_to_all(block, "col", 0, 0)
    later = make_blocks(
        list(range(2, 2 * phases)), (2 * phases - 2, S, S), order, reflectors, factors
    )
    later, blocks = lax.optimization_barrier((later, blocks))
    halo = from_next(blocks[:2, ::2])
    parts = [later] + [
        lax.ppermute(later, "col", [(c, (c + d) % cols) for c in range(cols)]) for d in (1, 2, 3)
    ]
    window = eigvecs
    for n in range(phases):
        partial, window, response = call(
            functools.partial(phase_kernel, n, max(n - 1, 0)),
            [(S, 2 * S), (2 * H, columns), (H, S)],
            order, offsets, window, halo_rows, blocks, halo, smem=2,
            scratch=[pltpu.VMEM((2 * H, S), F32)],
        )
        other = swap(partial)
        share = call(join_kernel, (SHARE, columns), partial, other)
        shares = lax.all_gather(share, ("z", "core"), axis=0, tiled=True)
        carry, at_chip, out = call(
            enter_kernel,
            [(S, columns), (S, S), (PLANES, 2 * SHARE, S)],
            other, shares,
        )
        if n == 0:
            out, parts = lax.optimization_barrier((out, parts))
        crossing = lax.all_to_all(out, "x", 0, 0)
        if n == 0:
            crossing, parts = lax.optimization_barrier((crossing, parts))
            blocks, head = call(
                pick_kernel,
                [(cols, 2 * phases - 2, S, S), (2, phases - 1, S, S)],
                *parts,
            )
            halo = from_next(head)
        window = call(
            functools.partial(finish_kernel, n), (2 * H, columns),
            order, offsets, carry, at_chip, crossing, response, window, smem=2,
        )
        if n < phases - 1:
            halo_rows = from_next(window[:H])
    before = from_previous(window[H : H + W])
    return call(
        functools.partial(last_kernel, phases - 1), (H, columns),
        order, offsets, window, before, smem=2,
    )


def solution(mesh):
    torus = Mesh(mesh.devices.reshape(PLANES, CHIPS, 2, mesh.shape["col"]), ROW_COL)
    placed = (P(ROW, "col"), P(None, ROW_COL, None, None), P(None, ROW_COL, None, None), P(), P())
    return jax.shard_map(
        local, mesh=torus, in_specs=placed, out_specs=P(ROW, "col"), check_vma=False
    )
```

```python
import functools

import jax
import jax.numpy as jnp
from jax import lax
from jax.experimental import pallas as pl
from jax.experimental.pallas import tpu as pltpu
from jax.sharding import Mesh
from jax.sharding import PartitionSpec as P

ROW = ("x", "z", "core")
ROW_COL = ("x", "z", "core", "col")
W = 64
S = 2 * W
H = 4 * W
CHIPS, PLANES = 8, 4
SHARE = (S + S - W // 2) // 2
F32 = jnp.float32


def exact(a, b, axis):
    return lax.dot_general(
        a,
        b,
        (((axis,), (0,)), ((), ())),
        precision=lax.Precision.HIGHEST,
        preferred_element_type=F32,
    )


def halves(a):
    high = a.astype(jnp.bfloat16)
    return high, (a - high.astype(F32)).astype(jnp.bfloat16)


def dot(a, b):
    a_high, a_low = halves(a)
    b_high, b_low = halves(b)
    return jnp.dot(
        jnp.concatenate([a_high, a_high, a_low], 1),
        jnp.concatenate([b_high, b_low, b_high], 0),
        preferred_element_type=F32,
    )


def call(body, outs, *args, smem=0, hbm=0, scratch=(), flops=20_000_000, limit=32):
    spaces = [pl.BlockSpec(memory_space=pltpu.SMEM)] * smem
    spaces += [pl.BlockSpec(memory_space=pltpu.HBM)] * hbm
    spaces += [pl.BlockSpec(memory_space=pltpu.VMEM)] * (len(args) - smem - hbm)
    single = not isinstance(outs, list)
    shapes = [jax.ShapeDtypeStruct(o, F32) for o in ([outs] if single else outs)]
    specs = [pl.BlockSpec(memory_space=pltpu.VMEM)] * len(shapes)
    return pl.pallas_call(
        body,
        out_shape=shapes[0] if single else shapes,
        in_specs=spaces,
        out_specs=specs[0] if single else specs,
        scratch_shapes=list(scratch),
        cost_estimate=pl.CostEstimate(flops=flops, bytes_accessed=1_000_000, transcendentals=0),
        compiler_params=pltpu.CompilerParams(vmem_limit_bytes=limit * 1024 * 1024),
    )(*args)


def eye(n):
    r = lax.broadcasted_iota(jnp.int32, (n, n), 0)
    c = lax.broadcasted_iota(jnp.int32, (n, n), 1)
    return jnp.where(r == c, 1.0, 0.0).astype(F32)


def row_index():
    x, z, core = lax.axis_index("x"), lax.axis_index("z"), lax.axis_index("core")
    return (x * CHIPS + z) * 2 + core


def is_last(g):
    return g == PLANES * CHIPS * 2 - 1


def block_kernel(positions, order, house, tri, out, v, t, sems):
    copies = []
    for i, p in enumerate(positions):
        copies.append(pltpu.make_async_copy(house.at[order[p], 0], v.at[i], sems.at[i, 0]))
        copies.append(pltpu.make_async_copy(tri.at[order[p], 0], t.at[i], sems.at[i, 1]))
    for copy in copies:
        copy.start()
    for copy in copies:
        copy.wait()
    for i in range(len(positions)):
        h = eye(S) - exact(v[i], exact(t[i], v[i], 1), 0)
        if len(out.shape) == 4:
            for c in range(out.shape[0]):
                out[c, i] = h
        else:
            out[i] = h


def make_blocks(positions, shape, order, house, tri):
    count = len(positions)
    return call(
        functools.partial(block_kernel, positions), shape, order, house, tri, smem=1, hbm=2,
        limit=60,
        scratch=[
            pltpu.VMEM((count, W, S), F32),
            pltpu.VMEM((count, W, W), F32),
            pltpu.SemaphoreType.DMA((count, 2)),
        ],
    )


def pick_kernel(part0, part1, part2, part3, blocks, head):
    parts = (part0, part1, part2, part3)
    for j in range(4):
        back = lax.rem(lax.axis_index("col") + 4 - j, 4)
        for i in range(part0.shape[0]):
            block = part0[i]
            for k in (1, 2, 3):
                block = jnp.where(back == k, parts[k][i], block)
            blocks[j, i] = block
            if j < 2 and i % 2 == 0:
                head[j, i // 2] = block


def chain(wins, blocks, count, offset, carry, probe):
    wide = len(wins) * S
    used = [win for k, win in enumerate(wins) if k * S < probe]
    added, steps = [], []
    for j in range(count):
        rest = [win[pl.ds(offset + (j + 1) * W, W), :] for win in used]
        rest = jnp.concatenate(rest, 1)
        if j == 0:
            start = [carry] + [jnp.zeros((W, S), F32)] * (len(used) - 1)
            start = jnp.concatenate(start, 1)
            add = dot(blocks(0), jnp.concatenate([start, rest], 0))
        else:
            add = dot(blocks(j)[:, W:], rest)
        add = add[:, :probe]
        blank = [jnp.zeros((W, wide - probe - W), F32)] if wide - probe - W else []
        steps.append(jnp.concatenate([add[W:], blocks(j)[W:, :W]] + blank, 1))
        zero = jnp.zeros((S, wide - probe), F32)
        added.append(jnp.concatenate([add, zero], 1))

    def join(later, earlier):
        own = jnp.concatenate([later[:, :probe], jnp.zeros((W, wide - probe), F32)], 1)
        return dot(later[:, probe : probe + W], earlier) + own

    pairs = [join(steps[k + 1], steps[k]) for k in range(0, count, 2)]
    r = lax.broadcasted_iota(jnp.int32, (W, wide), 0)
    c = lax.broadcasted_iota(jnp.int32, (W, wide), 1)
    entering = [jnp.where(r + probe == c, 1.0, 0.0).astype(F32), steps[0], pairs[0]]
    entering += [join(steps[2], pairs[0]), join(pairs[1], pairs[0])]
    if count == 6:
        entering.append(join(steps[4], entering[4]))
    for j in range(count):
        done = dot(blocks(j)[:W, :W], entering[j]) + added[j][:W]
        for k, win in enumerate(wins):
            win[pl.ds(offset + j * W, W), :] = done[:, k * S : (k + 1) * S]
    return entering[4]


def phase_kernel(n, i, order, offsets, own, halo_rows, blocks, halo, partial, window, response, win):
    g = row_index()
    last, leading = is_last(g), g == 0
    off_a, off_b = offsets[order[2 * n]], offsets[order[2 * n + 1]]
    win[...] = jnp.zeros_like(win)
    window[:H, :] = own[:H, :]
    if n:
        before = offsets[order[2 * n - 1]]
        rows = lax.broadcasted_iota(jnp.int32, (H, 1), 0)
        window[H:, :] = jnp.where((rows < before) & ~last, own[H:, :], halo_rows[...])
    else:
        window[H:, :] = halo_rows[...]
    wins = [window, win]

    def first(j):
        return blocks[j, 2 * i] if j < 4 else halo[j - 4, i]

    def second(j):
        return blocks[j, 2 * i + 1]

    carry = jnp.where(leading, window[pl.ds(off_a, W), :], 0.0)
    partial[:W] = chain(wins, first, 6, off_a, carry, S)
    for part in wins:
        part[H:, :] = jnp.where(last, 0.0, part[H:, :])
    carry = jnp.where(leading, window[pl.ds(off_b, W), :], 0.0)
    partial[W:] = chain(wins, second, 4, off_b, carry, S + W)
    response[...] = win[pl.ds(off_b, H), :]


def packed(step):
    return jnp.concatenate([step[:W // 2, :W], step[W // 2 : W, :W]], 1)


def unpacked(top, bottom):
    square = jnp.concatenate([top[:, :W], top[:, W:]], 0)
    return jnp.concatenate([jnp.concatenate([square, jnp.zeros_like(square)], 1), bottom], 0)


CUT = SHARE - W // 2


def join_kernel(partial, other, share):
    upper = lax.axis_index("core") == 1
    front = jnp.where(upper, other[...], partial[...])
    back = jnp.where(upper, partial[...], other[...])
    value = dot(back[:, S:], front)
    rows, step = value[:, :S] + back[:, :S], value[:, S:]
    low = jnp.concatenate([packed(step), rows[:CUT]], 0)
    high = jnp.concatenate([step[W:], rows[CUT:]], 0)
    share[...] = jnp.where(upper, high, low)


def after(later, earlier):
    own = jnp.concatenate([later[:, :S], jnp.zeros((S, S), F32)], 1)
    return dot(later[:, S:], earlier) + own


def enter_kernel(other, shares, carry, at_chip, out):
    z, upper = lax.axis_index("z"), lax.axis_index("core") == 1
    same = jnp.concatenate([jnp.zeros((S, S), F32), eye(S)], 1)
    chips = []
    for k in range(CHIPS):
        low = shares[2 * k * SHARE : (2 * k + 1) * SHARE]
        high = shares[(2 * k + 1) * SHARE : (2 * k + 2) * SHARE]
        step = unpacked(low[: W // 2], high[:W])
        rows = jnp.concatenate([low[W // 2 :], high[W:]], 0)
        chips.append(jnp.concatenate([rows, step], 1))
    pairs = [after(chips[k + 1], chips[k]) for k in range(0, CHIPS, 2)]
    four, two, one = z >= 4, lax.rem(z, 4) >= 2, lax.rem(z, 2) == 1
    single = jnp.where(
        four, jnp.where(two, chips[6], chips[4]), jnp.where(two, chips[2], chips[0])
    )
    nearest = after(jnp.where(upper, other[...], same), jnp.where(one, single, same))
    pair = jnp.where(two, jnp.where(four, pairs[2], pairs[0]), same)
    front = after(pairs[1], pairs[0])
    back = after(pairs[3], pairs[2])
    here = after(after(nearest, pair), jnp.where(four, front, same))
    carry[...] = here[:, :S]
    at_chip[...] = here[:, S:]
    total = after(back, front)
    value = jnp.concatenate([total[:, :S], packed(total[:, S:]), total[W:, S:]], 0)
    for x in range(PLANES):
        out[x] = value


def finish_kernel(n, order, offsets, carry, at_chip, crossing, response, window, out):
    x = lax.axis_index("x")
    off_b = offsets[order[2 * n + 1]]

    def plane(k):
        step = unpacked(crossing[k, S : S + W // 2], crossing[k, S + W // 2 :])
        return crossing[k, :S], step

    (rows0, _), (rows1, step1), (rows2, step2) = plane(0), plane(1), plane(2)
    out[...] = window[...]
    entry = jnp.where(x == 0, 0.0, at_chip[...])
    third = dot(entry, jnp.concatenate([rows2, step2], 1))
    through = jnp.where(x == 3, third[:, S:], entry)
    arrived = jnp.where(x == 1, rows0, rows1 + dot(step1, rows0))
    total = carry[...] + dot(through, arrived) + jnp.where(x == 3, third[:, :S], 0.0)
    rows = pl.ds(off_b, H)
    out[rows, :] = out[rows, :] + dot(response[...], total)


def last_kernel(n, order, offsets, window, before, out):
    g = row_index()
    off_b = offsets[order[2 * n + 1]]
    rows = lax.broadcasted_iota(jnp.int32, (W, 1), 0)
    out[...] = window[:H, :]
    out[:W, :] = jnp.where((rows < off_b) & (g != 0), before[...], window[:W, :])


def from_next(block):
    size = lax.axis_size(ROW)
    return lax.ppermute(block, ROW, [(i + 1, i) for i in range(size - 1)])


def from_previous(block):
    size = lax.axis_size(ROW)
    return lax.ppermute(block, ROW, [(i, i + 1) for i in range(size - 1)])


def swap(block):
    return lax.ppermute(block, "core", [(0, 1), (1, 0)])


def local(eigvecs, reflectors, factors, order, offsets):
    columns = eigvecs.shape[1]
    phases = order.shape[0] // 2
    cols = lax.axis_size("col")

    halo_rows = from_next(eigvecs)
    reflectors = jnp.swapaxes(reflectors, 2, 3)
    block = make_blocks([0, 1], (cols, 2, S, S), order, reflectors, factors)
    blocks = lax.all_to_all(block, "col", 0, 0)
    later = make_blocks(
        list(range(2, 2 * phases)), (2 * phases - 2, S, S), order, reflectors, factors
    )
    later, blocks = lax.optimization_barrier((later, blocks))
    halo = from_next(blocks[:2, ::2])
    parts = [later] + [
        lax.ppermute(later, "col", [(c, (c + d) % cols) for c in range(cols)]) for d in (1, 2, 3)
    ]
    window = eigvecs
    for n in range(phases):
        partial, window, response = call(
            functools.partial(phase_kernel, n, max(n - 1, 0)),
            [(S, 2 * S), (2 * H, columns), (H, S)],
            order, offsets, window, halo_rows, blocks, halo, smem=2,
            scratch=[pltpu.VMEM((2 * H, S), F32)],
        )
        other = swap(partial)
        share = call(join_kernel, (SHARE, columns), partial, other)
        shares = lax.all_gather(share, ("z", "core"), axis=0, tiled=True)
        carry, at_chip, out = call(
            enter_kernel,
            [(S, columns), (S, S), (PLANES, 2 * SHARE, S)],
            other, shares,
        )
        if n == 0:
            out, parts = lax.optimization_barrier((out, parts))
        crossing = lax.all_to_all(out, "x", 0, 0)
        if n == 0:
            crossing, parts = lax.optimization_barrier((crossing, parts))
            blocks, head = call(
                pick_kernel,
                [(cols, 2 * phases - 2, S, S), (2, phases - 1, S, S)],
                *parts,
            )
            halo = from_next(head)
        window = call(
            functools.partial(finish_kernel, n), (2 * H, columns),
            order, offsets, carry, at_chip, crossing, response, window, smem=2,
        )
        if n < phases - 1:
            halo_rows = from_next(window[:H])
    before = from_previous(window[H : H + W])
    return call(
        functools.partial(last_kernel, phases - 1), (H, columns),
        order, offsets, window, before, smem=2,
    )


def solution(mesh):
    torus = Mesh(mesh.devices.reshape(PLANES, CHIPS, 2, mesh.shape["col"]), ROW_COL)
    placed = (P(ROW, "col"), P(None, ROW_COL, None, None), P(None, ROW_COL, None, None), P(), P())
    return jax.shard_map(
        local, mesh=torus, in_specs=placed, out_specs=P(ROW, "col"), check_vma=False
    )
```
